256 devices in a mesh: epoch: 16 (over y, x), blend: 16 (over z, core).
Axes of the slice: x: 4, y: 4, z: 8, core: 2. Of those that a mesh axis runs over, the one named last changes fastest.
Arguments:
- visit_flux: bfloat16 [64, 64, 6, 16384], P('epoch', None, None, 'blend'), may hold values from -6 to 6
- visit_precision: bfloat16 [64, 64, 6, 16384], P('epoch', None, None, 'blend'), may hold values from 0.25 to 4
- visit_live: int32 [64, 64], P('epoch'), may hold values 0 or 1
- footprint: int32 [64, 8, 16384], P('blend', None, 'epoch'), may hold values 0 or 1
- source_count: int32 [64], P('blend'), may hold values from 1 to 8
- spectra_init: float32 [64, 8, 6], P('blend'), may hold values from 0.2 to 1.2
- morphology_init: float32 [64, 8, 16384], P('blend', None, 'epoch'), may hold values from 0 to 0.25
Outputs:
- coadd_flux: float32 [64, 6, 16384], P('blend', None, 'epoch')
- spectra: float32 [64, 8, 6], P('blend')
- morphology: float32 [64, 8, 16384], P('blend', None, 'epoch')
The draws below stay inside these ranges and needn't reach their ends.
All inputs are finite; a program needn't handle non-finite values. No bound on the sum of `visit_live` or of `footprint` on one device may be relied on, other than what follows from the above.
Results may differ from the reference program's by a relative error of at most 0.0003.
Values sent between devices are 32-bit elements; how exact they have to be, the bound alone decides.
No kernel may reach another device: no remote copies, remote signals or barrier semaphores. Data moves between devices by JAX's collectives and lax.ppermute only.
A program may use at most 64 MiB of HBM per device.

```python
import math
import jax
import jax.numpy as jnp
from jax import lax

PIX = 16384
BANDS = 6
SRC = 8
ITERS = 2
EPOCHS = 64
BLENDS = 64


def with_ends(array, key, smallest, largest):
    dims = array.shape
    place = [jax.random.randint(jax.random.fold_in(key, axis), (), 0, dims[axis]) for axis in range(len(dims))]
    array = array.at[tuple(place)].set(smallest)
    longest = dims.index(max(dims))
    place[longest] = (place[longest] + 1) % dims[longest]
    return array.at[tuple(place)].set(largest)


def shard_levels(rng, shape, pieces, low, top_value):
    def one(position, blocks):
        draws = jax.random.uniform(jax.random.fold_in(jax.random.fold_in(rng, 6), position), (blocks,), jnp.float32, low / len(pieces), top_value / len(pieces))
        return jnp.repeat(jnp.exp(draws), shape[position] // blocks).reshape((-1,) + (1,) * (len(shape) - position - 1))

    gain = one(*pieces[0])
    for cut in pieces[1:]:
        gain = gain * one(*cut)
    return gain


def normal_values(own_key, extent, spread, bound, pieces=(), held_as=jnp.bfloat16):
    loudness = shard_levels(own_key, extent, pieces, -0.22, 0.18) if pieces else 1.0
    result = jax.random.normal(own_key, extent, jnp.float32) * spread * loudness
    return jnp.minimum(jnp.maximum(result, -bound), bound).astype(held_as)


def setup_inputs(seed: int = 0) -> dict:
    key_of = jax.random.split(jax.random.key(seed), 8)
    return {
        "visit_flux": normal_values(key_of[0], (EPOCHS, BLENDS, BANDS, PIX), 1.0, 6.0, ((0, 16), (3, 16))),
        "visit_precision": jnp.clip(jnp.exp(math.log(4.0) - 2.7725887 * jax.random.uniform(key_of[1], (EPOCHS, BLENDS, BANDS, PIX), jnp.float32) ** shard_levels(key_of[1], (EPOCHS, BLENDS, BANDS, PIX), ((0, 16), (3, 16)), -0.2, 0.2)), 0.25, 4.0).astype(jnp.bfloat16),
        "visit_live": with_ends((jax.random.randint(key_of[2], (EPOCHS, BLENDS), 0, 4) < 3).astype(jnp.int32), jax.random.fold_in(key_of[2], 1), 0, 1),
        "footprint": with_ends((jax.random.randint(key_of[3], (BLENDS, SRC, PIX), 0, 2) < 1).astype(jnp.int32), jax.random.fold_in(key_of[3], 1), 0, 1),
        "source_count": with_ends(jax.random.randint(key_of[4], (BLENDS,), 1, SRC + 1), jax.random.fold_in(key_of[4], 1), 1, SRC).astype(jnp.int32),
        "spectra_init": jnp.clip(0.2 + 1 * jax.random.uniform(key_of[5], (BLENDS, SRC, BANDS), jnp.float32) ** shard_levels(key_of[5], (BLENDS, SRC, BANDS), ((0, 16),), -0.2, 0.2), 0.2, 1.2),
        "morphology_init": jnp.clip(0.25 * jax.random.uniform(key_of[6], (BLENDS, SRC, PIX), jnp.float32) ** shard_levels(key_of[6], (BLENDS, SRC, PIX), ((0, 16), (2, 16)), -0.2, 0.2), 0.0, 0.25),
    }


def reference(visit_flux, visit_precision, visit_live, footprint, source_count, spectra_init, morphology_init):
    def accumulate(totals, visit):
        flux_one, precision_one, live_one = visit
        weights = precision_one.astype(jnp.float32) * live_one.astype(jnp.float32)[:, None, None]
        return (totals[0] + weights * flux_one.astype(jnp.float32), totals[1] + weights), None

    zeros = jnp.zeros(visit_flux.shape[1:], jnp.float32)
    (numerator, weight_sum), _ = lax.scan(accumulate, (zeros, zeros), (visit_flux, visit_precision, visit_live))
    coadd_flux = numerator / (1.0 + weight_sum)
    coverage = weight_sum / (1.0 + weight_sum)
    source_live = (jnp.arange(SRC, dtype=jnp.int32)[None, :] < source_count[:, None]).astype(jnp.float32)
    footprint_mask = footprint.astype(jnp.float32) * source_live[:, :, None]
    live_count = source_count.astype(jnp.float32)
    morphology = morphology_init * footprint_mask
    spectra = spectra_init
    highest = lax.Precision.HIGHEST
    for iteration in range(ITERS):
        blend_model = jnp.einsum("bkc,bkp->bcp", spectra, morphology, precision=highest)
        residual = coverage * (coadd_flux - blend_model)
        morph_grad = jnp.einsum("bkc,bcp->bkp", spectra, residual, precision=highest)
        morph_step = 1.0 / (1.0 + live_count[:, None] * jnp.sum(spectra * spectra, axis=2))
        morphology = jnp.maximum(0.0, morphology + morph_grad * morph_step[:, :, None]) * footprint_mask
        blend_model = jnp.einsum("bkc,bkp->bcp", spectra, morphology, precision=highest)
        residual = coverage * (coadd_flux - blend_model)
        spectra_grad = jnp.einsum("bkp,bcp->bkc", morphology, residual, precision=highest)
        morph_norm = jnp.sum(morphology * morphology, axis=2)
        spectra = jnp.maximum(0.0, spectra + spectra_grad / (1.0 + live_count[:, None] * morph_norm)[:, :, None])
    return coadd_flux, spectra, morphology
```

```python
import jax
import jax.numpy as jnp
from jax import lax
from jax.experimental import pallas as pl
from jax.experimental.pallas import tpu as pltpu
from jax.sharding import PartitionSpec as P

ITERS = 2
F32 = jnp.float32
FIRST = (0, 2)
SECOND = (1, 3, 4, 5, 6, 7)
VMEM = pl.BlockSpec(memory_space=pltpu.VMEM)
ANY = pl.BlockSpec(memory_space=pl.ANY)


def visit_kernel(pairs, flux_ref, prec_ref, live_ref, *rest):
    outs, (flux_buf, prec_buf, sems) = rest[: 2 * len(pairs)], rest[2 * len(pairs) :]
    e = lax.axis_index("epoch")
    odd = lax.rem(e, 2) == 1
    visits, bands = flux_buf.shape[1], flux_buf.shape[2]
    width = flux_buf.shape[4]
    copies = []
    starts = []
    for n, j in enumerate(pairs):
        start = pl.multiple_of(lax.bitwise_xor(lax.div(e, 2), j) * 8, 8)
        starts.append(start)
        a = pltpu.make_async_copy(flux_ref.at[:, :, pl.ds(start, 8), :], flux_buf.at[n], sems.at[0, n])
        b = pltpu.make_async_copy(prec_ref.at[:, :, pl.ds(start, 8), :], prec_buf.at[n], sems.at[1, n])
        a.start()
        b.start()
        copies.append((a, b))
    low_rows = lax.broadcasted_iota(jnp.int32, (8, 128), 0) < 4
    for n in range(len(pairs)):
        for copy in copies[n]:
            copy.wait()
        lives = [live_ref[v, pl.ds(starts[n], 8), :] for v in range(visits)]
        even_out, odd_out = outs[2 * n], outs[2 * n + 1]

        def lane_tile(l, _, n=n, lives=lives, even_out=even_out, odd_out=odd_out):
            lanes = pl.ds(pl.multiple_of(l * 128, 128), 128)
            for cc in range(bands // 2):
                sums = []
                for c in (2 * cc, 2 * cc + 1):
                    num = jnp.zeros((8, 128), F32)
                    wsum = jnp.zeros((8, 128), F32)
                    for v in range(visits):
                        w = prec_buf[n, v, c, :, lanes].astype(F32) * lives[v]
                        num = num + w * flux_buf[n, v, c, :, lanes].astype(F32)
                        wsum = wsum + w
                    sums.append((num, wsum))
                for q in range(2):
                    first, second = sums[0][q], sums[1][q]
                    low = jnp.where(low_rows, first, pltpu.roll(second, 4, 0))
                    high = jnp.where(low_rows, pltpu.roll(first, 4, 0), second)
                    even_out[q * (bands // 2) + cc, :, lanes] = jnp.where(odd, high, low)
                    odd_out[q * (bands // 2) + cc, :, lanes] = jnp.where(odd, low, high)
            return 0

        lax.fori_loop(0, width // 128, lane_tile, 0)


def visit_sums(pairs, flux, prec, live):
    visits, bands, _, width = flux.shape
    piece = jax.ShapeDtypeStruct((bands, 8, width), F32)
    buf = pltpu.VMEM((len(pairs), visits, bands, 8, width), flux.dtype)
    work = visits * bands * 8 * len(pairs) * width
    return pl.pallas_call(
        lambda *refs: visit_kernel(pairs, *refs),
        out_shape=[piece] * (2 * len(pairs)),
        in_specs=[ANY, ANY, VMEM],
        out_specs=[VMEM] * (2 * len(pairs)),
        scratch_shapes=[buf, buf, pltpu.SemaphoreType.DMA((2, len(pairs)))],
        compiler_params=pltpu.CompilerParams(vmem_limit_bytes=20 * 2**20),
        cost_estimate=pl.CostEstimate(flops=8 * work, bytes_accessed=4 * work, transcendentals=0),
        name="visit_sums_%d" % len(pairs),
    )(flux, prec, live)


def spread(tile, n):
    return jnp.broadcast_to(tile[:, n : n + 1], tile.shape)


def step_body(s, many, coadd_ref, cover_ref, morph, mask_ref, morph_out, resid_ref, payload_ref):
    halves, width = resid_ref.shape[0], resid_ref.shape[2]
    slots = mask_ref.shape[0]
    sb = [[spread(s, cc * slots + k) for cc in range(halves)] for k in range(slots)]
    steps = []
    for k in range(slots):
        sq = sb[k][0] * sb[k][0]
        for cc in range(1, halves):
            sq = sq + sb[k][cc] * sb[k][cc]
        sq = sq + pltpu.roll(sq, 4, 0)
        steps.append(1.0 / (1.0 + many * sq))

    def residual(ms, cc, lanes):
        model = sb[0][cc] * ms[0]
        for k in range(1, slots):
            model = model + sb[k][cc] * ms[k]
        return cover_ref[cc, :, lanes] * (coadd_ref[cc, :, lanes] - model)

    def lane_tile(l, _):
        lanes = pl.ds(pl.multiple_of(l * 128, 128), 128)
        ms = [morph[k, :, lanes] for k in range(slots)]
        rs = [residual(ms, cc, lanes) for cc in range(halves)]
        new = []
        for k in range(slots):
            grad = sb[k][0] * rs[0]
            for cc in range(1, halves):
                grad = grad + sb[k][cc] * rs[cc]
            grad = grad + pltpu.roll(grad, 4, 0)
            m = jnp.maximum(0.0, ms[k] + grad * steps[k]) * mask_ref[k, :, lanes]
            morph_out[k, :, lanes] = m
            new.append(m)
        for cc in range(halves):
            resid_ref[cc, :, lanes] = residual(new, cc, lanes)
        return 0

    lax.fori_loop(0, width // 128, lane_tile, 0)
    lane = lax.broadcasted_iota(jnp.int32, (8, 128), 1)
    total = jnp.zeros((8, 128), F32)
    rs = [resid_ref[cc] for cc in range(halves)]
    for k in range(slots):
        m = morph_out[k]
        for cc in range(halves):
            got = jnp.sum(m * rs[cc], axis=1, keepdims=True)
            total = jnp.where(lane == cc * slots + k, got, total)
        got = jnp.sum(m * m, axis=1, keepdims=True)
        total = jnp.where(lane == halves * slots + k, got, total)
    for n in range(payload_ref.shape[0]):
        payload_ref[n] = total


def spectra_step(s, many, arrived_ref, halves, slots):
    total = arrived_ref[0]
    for n in range(1, arrived_ref.shape[0]):
        total = total + arrived_ref[n]
    lane = lax.broadcasted_iota(jnp.int32, (8, 128), 1)
    norm = total
    for cc in range(halves):
        moved = pltpu.roll(total, 128 - (halves - cc) * slots, 1)
        norm = jnp.where((lane >= cc * slots) & (lane < (cc + 1) * slots), moved, norm)
    new = jnp.maximum(0.0, s + total / (1.0 + many * norm))
    return jnp.where(lane < halves * slots, new, 0.0)


def first_kernel(sums_ref, mask_ref, morph_ref, s_ref, many_ref, coadd_ref, cover_ref, morph_out, payload_ref, resid_ref):
    halves = coadd_ref.shape[0]
    width = coadd_ref.shape[2]

    def lane_tile(l, _):
        lanes = pl.ds(pl.multiple_of(l * 128, 128), 128)
        for cc in range(halves):
            wsum = sums_ref[halves + cc, :, lanes]
            below = 1.0 / (1.0 + wsum)
            coadd_ref[cc, :, lanes] = sums_ref[cc, :, lanes] * below
            cover_ref[cc, :, lanes] = wsum * below
        return 0

    lax.fori_loop(0, width // 128, lane_tile, 0)
    step_body(s_ref[...], many_ref[...], coadd_ref, cover_ref, morph_ref, mask_ref, morph_out, resid_ref, payload_ref)


def next_kernel(arrived_ref, s_ref, many_ref, coadd_ref, cover_ref, morph_ref, mask_ref, s_out, morph_out, payload_ref, resid_ref):
    halves, slots = coadd_ref.shape[0], mask_ref.shape[0]
    s = spectra_step(s_ref[...], many_ref[...], arrived_ref, halves, slots)
    s_out[...] = s
    step_body(s, many_ref[...], coadd_ref, cover_ref, morph_ref, mask_ref, morph_out, resid_ref, payload_ref)


def last_kernel(arrived_ref, s_ref, many_ref, out_ref):
    bands, owned, slots = out_ref.shape
    s = spectra_step(s_ref[...], many_ref[...], arrived_ref, bands // 2, slots)
    for c in range(bands):
        out_ref[c] = s[(c % 2) * owned : (c % 2 + 1) * owned, (c // 2) * slots : (c // 2 + 1) * slots]


def call(kernel, outs, args, scratch=(), name=None):
    return pl.pallas_call(
        kernel,
        out_shape=[jax.ShapeDtypeStruct(o, F32) for o in outs],
        in_specs=[VMEM] * len(args),
        out_specs=[VMEM] * len(outs),
        scratch_shapes=[pltpu.VMEM(s, F32) for s in scratch],
        compiler_params=pltpu.CompilerParams(vmem_limit_bytes=8 * 2**20),
        cost_estimate=pl.CostEstimate(flops=4_000_000, bytes_accessed=1_000_000, transcendentals=0),
        name=name,
    )(*args)


def on_device(visit_flux, visit_precision, visit_live, footprint, source_count, spectra_init, morphology_init):
    n_epoch, n_blend = lax.axis_size("epoch"), lax.axis_size("blend")
    owned, slots, width = footprint.shape
    bands = visit_flux.shape[2]
    halves = bands // 2
    flux = jnp.transpose(visit_flux, (0, 2, 1, 3))
    prec = jnp.transpose(visit_precision, (0, 2, 1, 3))
    live = jnp.broadcast_to(visit_live.astype(F32)[:, :, None], (*visit_live.shape, 128))
    pieces = [None] * n_epoch
    for pairs in (FIRST, SECOND):
        got = visit_sums(pairs, flux, prec, live)
        for n, j in enumerate(pairs):
            pieces[2 * j], pieces[2 * j + 1] = got[2 * n], got[2 * n + 1]
    total = pieces[0]
    for m in range(1, n_epoch):
        total = total + lax.ppermute(pieces[m], "epoch", [(e, e ^ m) for e in range(n_epoch)])
    swap = [(a * n_blend + b, b * n_blend + a) for a in range(n_epoch) for b in range(n_blend)]
    sums = lax.ppermute(total, ("epoch", "blend"), swap)

    source_live = (jnp.arange(slots, dtype=jnp.int32)[None, :] < source_count[:, None]).astype(F32)
    mask = footprint.astype(F32) * source_live[:, :, None]
    twice = lambda a: jnp.concatenate([a, a], axis=1)
    mask_t = twice(jnp.transpose(mask, (1, 0, 2)))
    morph_t = twice(jnp.transpose(morphology_init * mask, (1, 0, 2)))
    many = jnp.broadcast_to(jnp.tile(source_count.astype(F32), 2)[:, None], (8, 128))
    s = jnp.transpose(spectra_init.reshape(owned, slots, halves, 2), (3, 0, 2, 1)).reshape(2 * owned, halves * slots)
    s = jnp.pad(s, ((0, 0), (0, 128 - halves * slots)))

    tile3, tile8 = (halves, 8, width), (slots, 8, width)
    payload = (n_epoch, 8, 128)
    coadd, cover, morph, sent = call(
        first_kernel, [tile3, tile3, tile8, payload], [sums, mask_t, morph_t, s, many], [tile3], "deblend_first"
    )
    swap_all = lambda a: lax.all_to_all(a, "epoch", split_axis=0, concat_axis=0, tiled=True)
    s, morph, sent = call(
        next_kernel,
        [(8, 128), tile8, payload],
        [swap_all(sent), s, many, coadd, cover, morph, mask_t],
        [tile3],
        "deblend_next",
    )
    (spectra,) = call(last_kernel, [(bands, owned, slots)], [swap_all(sent), s, many], (), "deblend_last")
    coadd = jnp.transpose(coadd.reshape(bands, owned, width), (1, 0, 2))
    return coadd, jnp.transpose(spectra, (1, 2, 0)), jnp.transpose(morph[:, :owned], (1, 0, 2))


def solution(mesh):
    in_specs = (
        P("epoch", None, None, "blend"),
        P("epoch", None, None, "blend"),
        P("epoch", None),
        P("blend", None, "epoch"),
        P("blend"),
        P("blend", None, None),
        P("blend", None, "epoch"),
    )
    out_specs = (P("blend", None, "epoch"), P("blend", None, None), P("blend", None, "epoch"))
    return jax.shard_map(
        on_device, mesh=mesh, in_specs=in_specs, out_specs=out_specs, check_vma=False
    )
```

```python
import jax
import jax.numpy as jnp
from jax import lax
from jax.experimental import pallas as pl
from jax.experimental.pallas import tpu as pltpu
from jax.sharding import PartitionSpec as P

ITERS = 2
VISIT_VMEM = 20 * 2**20
F32 = jnp.float32
FIRST = [(2 * r, 0, ((0, r), (1, r))) for r in range(4)] + [(2 + p, 1, ((2, 2 * p), (2, 2 * p + 1))) for p in range(2)]
SECOND = [(2 * r + 1, 0, ((0, r), (1, r))) for r in range(4)] + [
    (2 * r + p, 1, ((n, 2 * p), (n, 2 * p + 1))) for n, r in ((2, 2), (3, 3), (4, 0)) for p in range(2)
]
VMEM = pl.BlockSpec(memory_space=pltpu.VMEM)
ANY = pl.BlockSpec(memory_space=pl.ANY)


def held_group(e, i):
    return 2 * ((e // 2 + 4 * (i % 2) - i // 2) % 8) + (e + i) % 2


def visit_kernel(tasks, n_out, after, flux_ref, prec_ref, live_ref, *rest):
    outs, (flux_buf, prec_buf, sems) = rest[after : after + n_out], rest[after + n_out :]
    e, i = lax.axis_index("epoch"), lax.axis_index("blend")
    odd = lax.rem(e + i, 2) == 1
    visits, bands = flux_buf.shape[1], flux_buf.shape[2]
    width = flux_buf.shape[4]
    copies = []
    starts = []
    for n, (j, half, _) in enumerate(tasks):
        pair = lax.rem(lax.bitwise_xor(lax.div(e, 2), j) + 4 * lax.rem(i, 2) + 8 - lax.div(i, 2), 8)
        start = pl.multiple_of(pair * 8, 8)
        starts.append(start)
        lanes = pl.ds(half * width, width)
        a = pltpu.make_async_copy(flux_ref.at[:, :, pl.ds(start, 8), lanes], flux_buf.at[n], sems.at[0, n])
        b = pltpu.make_async_copy(prec_ref.at[:, :, pl.ds(start, 8), lanes], prec_buf.at[n], sems.at[1, n])
        a.start()
        b.start()
        copies.append((a, b))
    low_rows = lax.broadcasted_iota(jnp.int32, (8, 128), 0) < 4
    for n, (_, _, ((out0, at0), (out1, at1))) in enumerate(tasks):
        for copy in copies[n]:
            copy.wait()
        lives = [live_ref[v, pl.ds(starts[n], 8), :] for v in range(visits)]

        def lane_tile(l, _, n=n, lives=lives, even=outs[out0].at[at0], uneven=outs[out1].at[at1]):
            lanes = pl.ds(pl.multiple_of(l * 128, 128), 128)
            for cc in range(bands // 2):
                sums = []
                for c in (2 * cc, 2 * cc + 1):
                    num = jnp.zeros((8, 128), F32)
                    wsum = jnp.zeros((8, 128), F32)
                    for v in range(visits):
                        w = prec_buf[n, v, c, :, lanes].astype(F32) * lives[v]
                        num = num + w * flux_buf[n, v, c, :, lanes].astype(F32)
                        wsum = wsum + w
                    sums.append((num, wsum))
                for q in range(2):
                    first, second = sums[0][q], sums[1][q]
                    low = jnp.where(low_rows, first, pltpu.roll(second, 4, 0))
                    high = jnp.where(low_rows, pltpu.roll(first, 4, 0), second)
                    even[q * (bands // 2) + cc, :, lanes] = jnp.where(odd, high, low)
                    uneven[q * (bands // 2) + cc, :, lanes] = jnp.where(odd, low, high)
            return 0

        lax.fori_loop(0, width // 128, lane_tile, 0)


def visit_sums(tasks, flux, prec, live, *after):
    visits, bands, _, width = flux.shape
    n_out = 1 + max(out for _, _, places in tasks for out, _ in places)
    piece = jax.ShapeDtypeStruct((4, bands, 8, width // 2), F32)
    buf = pltpu.VMEM((len(tasks), visits, bands, 8, width // 2), flux.dtype)
    work = visits * bands * 4 * len(tasks) * width
    return pl.pallas_call(
        lambda *refs: visit_kernel(tasks, n_out, len(after), *refs),
        out_shape=[piece] * n_out,
        in_specs=[ANY, ANY, VMEM] + [ANY] * len(after),
        out_specs=[VMEM] * n_out,
        scratch_shapes=[buf, buf, pltpu.SemaphoreType.DMA((2, len(tasks)))],
        compiler_params=pltpu.CompilerParams(vmem_limit_bytes=VISIT_VMEM),
        cost_estimate=pl.CostEstimate(flops=8 * work, bytes_accessed=4 * work, transcendentals=0),
        name="visit_sums_%d" % len(tasks),
    )(flux, prec, live, *after)


def join_kernel(*refs):
    ins, outs = refs[:4], refs[4:]
    for n, out in enumerate(outs):
        out[...] = (ins[0][n] + ins[1][n]) + (ins[2][n] + ins[3][n])


def spread(tile, n):
    return jnp.broadcast_to(tile[:, n : n + 1], tile.shape)


def step_body(s, many, coadd_ref, cover_ref, morph, mask_ref, morph_out, resid_ref, payload_ref):
    halves, width = resid_ref.shape[0], resid_ref.shape[2]
    slots = mask_ref.shape[0]
    sb = [[spread(s, cc * slots + k) for cc in range(halves)] for k in range(slots)]
    steps = []
    for k in range(slots):
        sq = sb[k][0] * sb[k][0]
        for cc in range(1, halves):
            sq = sq + sb[k][cc] * sb[k][cc]
        sq = sq + pltpu.roll(sq, 4, 0)
        steps.append(1.0 / (1.0 + many * sq))

    def residual(ms, cc, lanes):
        model = sb[0][cc] * ms[0]
        for k in range(1, slots):
            model = model + sb[k][cc] * ms[k]
        return cover_ref[cc, :, lanes] * (coadd_ref[cc, :, lanes] - model)

    def lane_tile(l, _):
        lanes = pl.ds(pl.multiple_of(l * 128, 128), 128)
        ms = [morph[k, :, lanes] for k in range(slots)]
        rs = [residual(ms, cc, lanes) for cc in range(halves)]
        new = []
        for k in range(slots):
            grad = sb[k][0] * rs[0]
            for cc in range(1, halves):
                grad = grad + sb[k][cc] * rs[cc]
            grad = grad + pltpu.roll(grad, 4, 0)
            m = jnp.maximum(0.0, ms[k] + grad * steps[k]) * mask_ref[k, :, lanes]
            morph_out[k, :, lanes] = m
            new.append(m)
        for cc in range(halves):
            resid_ref[cc, :, lanes] = residual(new, cc, lanes)
        return 0

    lax.fori_loop(0, width // 128, lane_tile, 0)
    lane = lax.broadcasted_iota(jnp.int32, (8, 128), 1)
    total = jnp.zeros((8, 128), F32)
    rs = [resid_ref[cc] for cc in range(halves)]
    for k in range(slots):
        m = morph_out[k]
        for cc in range(halves):
            got = jnp.sum(m * rs[cc], axis=1, keepdims=True)
            total = jnp.where(lane == cc * slots + k, got, total)
        got = jnp.sum(m * m, axis=1, keepdims=True)
        total = jnp.where(lane == halves * slots + k, got, total)
    for n in range(payload_ref.shape[0]):
        payload_ref[n] = total


def spectra_step(s, many, arrived_ref, halves, slots):
    total = arrived_ref[0]
    for n in range(1, arrived_ref.shape[0]):
        total = total + arrived_ref[n]
    lane = lax.broadcasted_iota(jnp.int32, (8, 128), 1)
    norm = total
    for cc in range(halves):
        moved = pltpu.roll(total, 128 - (halves - cc) * slots, 1)
        norm = jnp.where((lane >= cc * slots) & (lane < (cc + 1) * slots), moved, norm)
    new = jnp.maximum(0.0, s + total / (1.0 + many * norm))
    return jnp.where(lane < halves * slots, new, 0.0)


def total_kernel(*refs):
    out = refs[8]
    width = out.shape[2] // 2
    for half in range(2):
        a, b, c, d = refs[4 * half : 4 * half + 4]
        out[:, :, half * width : (half + 1) * width] = (a[...] + b[...]) + (c[...] + d[...])


def first_kernel(sums_ref, mask_ref, morph_ref, s_ref, many_ref, coadd_ref, cover_ref, morph_out, payload_ref, resid_ref):
    halves = coadd_ref.shape[0]
    width = coadd_ref.shape[2]

    def lane_tile(l, _):
        lanes = pl.ds(pl.multiple_of(l * 128, 128), 128)
        for cc in range(halves):
            wsum = sums_ref[halves + cc, :, lanes]
            below = 1.0 / (1.0 + wsum)
            coadd_ref[cc, :, lanes] = sums_ref[cc, :, lanes] * below
            cover_ref[cc, :, lanes] = wsum * below
        return 0

    lax.fori_loop(0, width // 128, lane_tile, 0)
    step_body(s_ref[...], many_ref[...], coadd_ref, cover_ref, morph_ref, mask_ref, morph_out, resid_ref, payload_ref)


def next_kernel(arrived_ref, s_ref, many_ref, coadd_ref, cover_ref, morph_ref, mask_ref, s_out, morph_out, payload_ref, resid_ref):
    halves, slots = coadd_ref.shape[0], mask_ref.shape[0]
    s = spectra_step(s_ref[...], many_ref[...], arrived_ref, halves, slots)
    s_out[...] = s
    step_body(s, many_ref[...], coadd_ref, cover_ref, morph_ref, mask_ref, morph_out, resid_ref, payload_ref)


def last_kernel(arrived_ref, s_ref, many_ref, out_ref):
    bands, owned, slots = out_ref.shape
    s = spectra_step(s_ref[...], many_ref[...], arrived_ref, bands // 2, slots)
    for c in range(bands):
        out_ref[c] = s[(c % 2) * owned : (c % 2 + 1) * owned, (c // 2) * slots : (c // 2 + 1) * slots]


def call(kernel, outs, args, scratch=(), name=None):
    return pl.pallas_call(
        kernel,
        out_shape=[jax.ShapeDtypeStruct(o, F32) for o in outs],
        in_specs=[VMEM] * len(args),
        out_specs=[VMEM] * len(outs),
        scratch_shapes=[pltpu.VMEM(s, F32) for s in scratch],
        compiler_params=pltpu.CompilerParams(vmem_limit_bytes=8 * 2**20),
        cost_estimate=pl.CostEstimate(flops=4_000_000, bytes_accessed=1_000_000, transcendentals=0),
        name=name,
    )(*args)


def on_device(visit_flux, visit_precision, visit_live, footprint, source_count, spectra_init, morphology_init):
    n_epoch, n_blend = lax.axis_size("epoch"), lax.axis_size("blend")
    owned, slots, width = footprint.shape
    bands = visit_flux.shape[2]
    halves = bands // 2
    hop = lambda a, m: lax.ppermute(a, "epoch", [(e, e ^ m) for e in range(n_epoch)])

    flux = jnp.transpose(visit_flux, (0, 2, 1, 3))
    prec = jnp.transpose(visit_precision, (0, 2, 1, 3))
    live = jnp.broadcast_to(visit_live.astype(F32)[:, :, None], (*visit_live.shape, 128))
    a0, a1, b1 = visit_sums(FIRST, flux, prec, live)
    a1, b1 = hop(a1, 1), hop(b1, 4)
    a2, a3, b2, b3, b0 = visit_sums(SECOND, flux, prec, live, a0)
    a3, b3, a2, b2 = hop(a3, 3), hop(b3, 12), hop(a2, 2), hop(b2, 8)

    piece = (bands, 8, width // 2)
    a = call(join_kernel, [piece] * 4, [a0, a1, a3, a2], (), "join_a")
    b = call(join_kernel, [piece] * 4, [b0, b1, b3, b2], (), "join_b")
    pieces = [a[0]] + [hop(a[m], 4 * m) for m in (1, 3, 2)] + [b[0]] + [hop(b[m], m) for m in (1, 3, 2)]
    (total,) = call(total_kernel, [(bands, 8, width)], pieces, (), "total")
    home = [(e * n_blend + i, i * n_blend + held_group(e, i)) for e in range(n_epoch) for i in range(n_blend)]
    sums = lax.ppermute(total, ("epoch", "blend"), home)

    source_live = (jnp.arange(slots, dtype=jnp.int32)[None, :] < source_count[:, None]).astype(F32)
    mask = footprint.astype(F32) * source_live[:, :, None]
    twice = lambda a: jnp.concatenate([a, a], axis=1)
    mask_t = twice(jnp.transpose(mask, (1, 0, 2)))
    morph_t = twice(jnp.transpose(morphology_init * mask, (1, 0, 2)))
    many = jnp.broadcast_to(jnp.tile(source_count.astype(F32), 2)[:, None], (8, 128))
    s = jnp.transpose(spectra_init.reshape(owned, slots, halves, 2), (3, 0, 2, 1)).reshape(2 * owned, halves * slots)
    s = jnp.pad(s, ((0, 0), (0, 128 - halves * slots)))

    tile3, tile8 = (halves, 8, width), (slots, 8, width)
    payload = (n_epoch, 8, 128)
    coadd, cover, morph, sent = call(
        first_kernel, [tile3, tile3, tile8, payload], [sums, mask_t, morph_t, s, many], [tile3], "deblend_first"
    )
    swap_all = lambda a: lax.all_to_all(a, "epoch", split_axis=0, concat_axis=0, tiled=True)
    s, morph, sent = call(
        next_kernel,
        [(8, 128), tile8, payload],
        [swap_all(sent), s, many, coadd, cover, morph, mask_t],
        [tile3],
        "deblend_next",
    )
    (spectra,) = call(last_kernel, [(bands, owned, slots)], [swap_all(sent), s, many], (), "deblend_last")
    coadd = jnp.transpose(coadd.reshape(bands, owned, width), (1, 0, 2))
    return coadd, jnp.transpose(spectra, (1, 2, 0)), jnp.transpose(morph[:, :owned], (1, 0, 2))


def solution(mesh):
    in_specs = (
        P("epoch", None, None, "blend"),
        P("epoch", None, None, "blend"),
        P("epoch", None),
        P("blend", None, "epoch"),
        P("blend"),
        P("blend", None, None),
        P("blend", None, "epoch"),
    )
    out_specs = (P("blend", None, "epoch"), P("blend", None, None), P("blend", None, "epoch"))
    return jax.shard_map(
        on_device, mesh=mesh, in_specs=in_specs, out_specs=out_specs, check_vma=False
    )
```

```python
import jax
import jax.numpy as jnp
from jax import lax
from jax.experimental import pallas as pl
from jax.experimental.pallas import tpu as pltpu
from jax.sharding import PartitionSpec as P

ITERS = 2
VISIT_VMEM = 52 * 2**20
F32 = jnp.float32
VMEM = pl.BlockSpec(memory_space=pltpu.VMEM)
ANY = pl.BlockSpec(memory_space=pl.ANY)


def held_group(e, i):
    return 2 * ((e // 2 + 4 * (i % 2) - i // 2) % 8) + (e + i) % 2


def visit_kernel(first, flux_ref, prec_ref, live_ref, *rest):
    if first:
        outs, (live_out, flux_buf, prec_buf, live_buf, square, sems, live_sem) = rest[:8], rest[8:]
    else:
        outs, (flux_buf, prec_buf, sems) = rest[:8], rest[8:]
    e, i = lax.axis_index("epoch"), lax.axis_index("blend")
    odd = lax.rem(e + i, 2) == 1
    bands, visits, tiles = flux_buf.shape[:3]
    width = flux_buf.shape[4]
    base = 0 if first else bands
    copies = []
    if first:
        live_copy = pltpu.make_async_copy(live_ref, live_buf, live_sem)
        live_copy.start()
    for c in range(bands):
        row = []
        for v in range(visits):
            row.append(pltpu.make_async_copy(prec_ref.at[v, base + c], prec_buf.at[c, v], sems.at[0, c, v]))
            row.append(pltpu.make_async_copy(flux_ref.at[v, base + c], flux_buf.at[c, v], sems.at[1, c, v]))
        for copy in row:
            copy.start()
        copies.append(row)
    if first:
        live_copy.wait()
        square[...] = jnp.zeros(square.shape, F32)
        square[:visits, : 8 * tiles] = live_buf[...].astype(F32)
        turned = jnp.transpose(square[...])
        for v in range(visits):
            live_out[v] = jnp.broadcast_to(turned[: 8 * tiles, v : v + 1], (8 * tiles, 128)).reshape(tiles, 8, 128)
        live = live_out
    else:
        live = live_ref
    low_rows = lax.broadcasted_iota(jnp.int32, (8, 128), 0) < 4
    for c in range(bands):
        for copy in copies[c]:
            copy.wait()
        for j in range(tiles):
            pair = lax.rem(lax.bitwise_xor(lax.div(e, 2), j) + 4 * lax.rem(i, 2) + 8 - lax.div(i, 2), 8)
            lives = [live[v, pair] for v in range(visits)]
            x, y = 2 * (j % 2), j // 2
            (far0, far1), (at0, at1) = ((x, x + 1), (y, y)) if first else ((y, y), (x, x + 1))
            even, uneven = outs[2 * far0 + at0 // 2].at[at0 % 2], outs[2 * far1 + at1 // 2].at[at1 % 2]

            def lane_tile(l, _, c=c, pair=pair, lives=lives, even=even, uneven=uneven):
                lanes = pl.ds(pl.multiple_of(l * 128, 128), 128)
                num = wsum = None
                for v in range(visits):
                    w = prec_buf[c, v, pair, :, lanes].astype(F32) * lives[v]
                    n = w * flux_buf[c, v, pair, :, lanes].astype(F32)
                    num, wsum = (n, w) if v == 0 else (num + n, wsum + w)
                low = jnp.where(low_rows, num, pltpu.roll(wsum, 4, 0))
                high = jnp.where(low_rows, pltpu.roll(num, 4, 0), wsum)
                even[c, :, lanes] = jnp.where(odd, high, low)
                uneven[c, :, lanes] = jnp.where(odd, low, high)
                return 0

            lax.fori_loop(0, width // 128, lane_tile, 0, unroll=True)


def visit_sums(first, flux, prec, live):
    visits, bands, tiles, _, width = flux.shape
    half = bands // 2
    piece = jax.ShapeDtypeStruct((2, half, 8, width), F32)
    buf = pltpu.VMEM((half, visits, tiles, 8, width), flux.dtype)
    work = visits * half * tiles * 8 * width
    outs, scratch = [piece] * 8, [buf, buf, pltpu.SemaphoreType.DMA((2, half, visits))]
    if first:
        outs.append(jax.ShapeDtypeStruct((visits, tiles, 8, 128), F32))
        scratch[2:2] = [pltpu.VMEM(live.shape, live.dtype), pltpu.VMEM((128, 128), F32)]
        scratch.append(pltpu.SemaphoreType.DMA)
    return pl.pallas_call(
        lambda *refs: visit_kernel(first, *refs),
        out_shape=outs,
        in_specs=[ANY, ANY, ANY if first else VMEM],
        out_specs=[VMEM] * len(outs),
        scratch_shapes=scratch,
        compiler_params=pltpu.CompilerParams(vmem_limit_bytes=VISIT_VMEM),
        cost_estimate=pl.CostEstimate(flops=8 * work, bytes_accessed=4 * work, transcendentals=0),
        name="visit_first" if first else "visit_second",
    )(flux, prec, live)


def pass_kernel(a, b, c, d, low, high):
    low[...] = a[...] + b[...]
    high[...] = c[...] + d[...]


def join_kernel(*refs):
    ins, outs = refs[:6], refs[6:]
    for n, out in enumerate(outs):
        a, b, c = ins[3 * (n // 2) : 3 * (n // 2) + 3]
        out[...] = a[n % 2] + b[n % 2] + c[n % 2]


def spread(tile, n):
    return jnp.broadcast_to(tile[:, n : n + 1], tile.shape)


def step_body(s, many, coadd_ref, cover_ref, morph, mask_ref, morph_out, resid_ref, payload_ref):
    halves, width = resid_ref.shape[0], resid_ref.shape[2]
    slots = mask_ref.shape[0]
    sb = [[spread(s, cc * slots + k) for cc in range(halves)] for k in range(slots)]
    steps = []
    for k in range(slots):
        sq = sb[k][0] * sb[k][0]
        for cc in range(1, halves):
            sq = sq + sb[k][cc] * sb[k][cc]
        sq = sq + pltpu.roll(sq, 4, 0)
        steps.append(1.0 / (1.0 + many * sq))

    def residual(ms, cc, lanes):
        model = sb[0][cc] * ms[0]
        for k in range(1, slots):
            model = model + sb[k][cc] * ms[k]
        return cover_ref[cc, :, lanes] * (coadd_ref[cc, :, lanes] - model)

    def lane_tile(l, _):
        lanes = pl.ds(pl.multiple_of(l * 128, 128), 128)
        ms = [morph[k, :, lanes] for k in range(slots)]
        rs = [residual(ms, cc, lanes) for cc in range(halves)]
        new = []
        for k in range(slots):
            grad = sb[k][0] * rs[0]
            for cc in range(1, halves):
                grad = grad + sb[k][cc] * rs[cc]
            grad = grad + pltpu.roll(grad, 4, 0)
            m = jnp.maximum(0.0, ms[k] + grad * steps[k]) * mask_ref[k, :, lanes]
            morph_out[k, :, lanes] = m
            new.append(m)
        for cc in range(halves):
            resid_ref[cc, :, lanes] = residual(new, cc, lanes)
        return 0

    lax.fori_loop(0, width // 128, lane_tile, 0)
    lane = lax.broadcasted_iota(jnp.int32, (8, 128), 1)
    total = jnp.zeros((8, 128), F32)
    rs = [resid_ref[cc] for cc in range(halves)]
    for k in range(slots):
        m = morph_out[k]
        for cc in range(halves):
            got = jnp.sum(m * rs[cc], axis=1, keepdims=True)
            total = jnp.where(lane == cc * slots + k, got, total)
        got = jnp.sum(m * m, axis=1, keepdims=True)
        total = jnp.where(lane == halves * slots + k, got, total)
    for n in range(payload_ref.shape[0]):
        payload_ref[n] = total


def spectra_step(s, many, arrived_ref, halves, slots):
    total = arrived_ref[0]
    for n in range(1, arrived_ref.shape[0]):
        total = total + arrived_ref[n]
    lane = lax.broadcasted_iota(jnp.int32, (8, 128), 1)
    norm = total
    for cc in range(halves):
        moved = pltpu.roll(total, 128 - (halves - cc) * slots, 1)
        norm = jnp.where((lane >= cc * slots) & (lane < (cc + 1) * slots), moved, norm)
    new = jnp.maximum(0.0, s + total / (1.0 + many * norm))
    return jnp.where(lane < halves * slots, new, 0.0)


def total_kernel(*refs):
    out = refs[8]
    half = out.shape[0] // 2
    for n in range(2):
        a, b, c, d = refs[4 * n : 4 * n + 4]
        out[n * half : (n + 1) * half] = (a[...] + b[...]) + (c[...] + d[...])


def first_kernel(
    sums_ref, mask_ref, morph_ref, s_ref, many_ref, coadd_ref, cover_ref, morph_out, payload_ref, resid_ref
):
    halves, width = coadd_ref.shape[0], coadd_ref.shape[2]
    low_rows = lax.broadcasted_iota(jnp.int32, (8, 128), 0) < 4

    def lane_tile(l, _):
        lanes = pl.ds(pl.multiple_of(l * 128, 128), 128)
        got = [sums_ref[n, :, lanes] for n in range(2 * halves)]
        for cc in range(halves):
            even, uneven = got[2 * cc], got[2 * cc + 1]
            num = jnp.where(low_rows, even, pltpu.roll(uneven, 4, 0))
            wsum = jnp.where(low_rows, pltpu.roll(even, 4, 0), uneven)
            below = 1.0 / (1.0 + wsum)
            coadd_ref[cc, :, lanes] = num * below
            cover_ref[cc, :, lanes] = wsum * below
        return 0

    lax.fori_loop(0, width // 128, lane_tile, 0)
    step_body(s_ref[...], many_ref[...], coadd_ref, cover_ref, morph_ref, mask_ref, morph_out, resid_ref, payload_ref)


def next_kernel(arrived_ref, s_ref, many_ref, coadd_ref, cover_ref, morph_ref, mask_ref, s_out, morph_out, payload_ref, resid_ref):
    halves, slots = coadd_ref.shape[0], mask_ref.shape[0]
    s = spectra_step(s_ref[...], many_ref[...], arrived_ref, halves, slots)
    s_out[...] = s
    step_body(s, many_ref[...], coadd_ref, cover_ref, morph_ref, mask_ref, morph_out, resid_ref, payload_ref)


def last_kernel(arrived_ref, s_ref, many_ref, out_ref):
    bands, owned, slots = out_ref.shape
    s = spectra_step(s_ref[...], many_ref[...], arrived_ref, bands // 2, slots)
    for c in range(bands):
        out_ref[c] = s[(c % 2) * owned : (c % 2 + 1) * owned, (c // 2) * slots : (c // 2 + 1) * slots]


def call(kernel, outs, args, scratch=(), name=None):
    return pl.pallas_call(
        kernel,
        out_shape=[jax.ShapeDtypeStruct(o, F32) for o in outs],
        in_specs=[VMEM] * len(args),
        out_specs=[VMEM] * len(outs),
        scratch_shapes=[pltpu.VMEM(s, F32) for s in scratch],
        compiler_params=pltpu.CompilerParams(vmem_limit_bytes=8 * 2**20),
        cost_estimate=pl.CostEstimate(flops=4_000_000, bytes_accessed=1_000_000, transcendentals=0),
        name=name,
    )(*args)


def on_device(visit_flux, visit_precision, visit_live, footprint, source_count, spectra_init, morphology_init):
    n_epoch, n_blend = lax.axis_size("epoch"), lax.axis_size("blend")
    owned, slots, width = footprint.shape
    bands = visit_flux.shape[2]
    halves = bands // 2
    hop = lambda a, m: lax.ppermute(a, "epoch", [(e, e ^ m) for e in range(n_epoch)])

    tiled = lambda a: jnp.transpose(a, (0, 2, 1, 3)).reshape(a.shape[0], bands, a.shape[1] // 8, 8, a.shape[3])
    flux, prec = tiled(visit_flux), tiled(visit_precision)
    both_ways = lambda a, b, step: (hop(a, step), hop(b, 3 * step))
    *a, live = visit_sums(True, flux, prec, visit_live)
    b = visit_sums(False, flux, prec, live)
    a_far = both_ways(a[4], a[5], 1)
    a_near = both_ways(a[2], a[7], 1)
    b_far = both_ways(b[4], b[5], 4)
    b_near = both_ways(b[2], b[7], 4)
    two = (2, halves, 8, width)
    a_last = both_ways(*call(pass_kernel, [two] * 2, [a[3], a_far[1], a[6], a_far[0]], (), "pass_a"), 1)
    b_last = both_ways(*call(pass_kernel, [two] * 2, [b[3], b_far[1], b[6], b_far[0]], (), "pass_b"), 4)

    piece = (halves, 8, width)
    home = [(e * n_blend + i, i * n_blend + held_group(e, i)) for e in range(n_epoch) for i in range(n_blend)]
    a = call(join_kernel, [piece] * 4, [a[0], a_near[0], a_last[1], a[1], a_near[1], a_last[0]], (), "join_a")
    a = [a[0]] + [hop(a[m], 4 * m) for m in (1, 3, 2)]
    b = call(join_kernel, [piece] * 4, [b[0], b_near[0], b_last[1], b[1], b_near[1], b_last[0]], (), "join_b")
    b = [b[0]] + [hop(b[m], m) for m in (1, 3, 2)]
    (total,) = call(total_kernel, [(bands, 8, width)], [*a, *b], (), "total")
    sums = lax.ppermute(total, ("epoch", "blend"), home)

    source_live = (jnp.arange(slots, dtype=jnp.int32)[None, :] < source_count[:, None]).astype(F32)
    mask = footprint.astype(F32) * source_live[:, :, None]
    twice = lambda a: jnp.concatenate([a, a], axis=1)
    mask_t = twice(jnp.transpose(mask, (1, 0, 2)))
    morph_t = twice(jnp.transpose(morphology_init * mask, (1, 0, 2)))
    many = jnp.broadcast_to(jnp.tile(source_count.astype(F32), 2)[:, None], (8, 128))
    s = jnp.transpose(spectra_init.reshape(owned, slots, halves, 2), (3, 0, 2, 1)).reshape(2 * owned, halves * slots)
    s = jnp.pad(s, ((0, 0), (0, 128 - halves * slots)))

    tile3, tile8 = (halves, 8, width), (slots, 8, width)
    payload = (n_epoch, 8, 128)
    coadd, cover, morph, sent = call(
        first_kernel, [tile3, tile3, tile8, payload], [sums, mask_t, morph_t, s, many], [tile3], "deblend_first"
    )
    swap_all = lambda a: lax.all_to_all(a, "epoch", split_axis=0, concat_axis=0, tiled=True)
    s, morph, sent = call(
        next_kernel,
        [(8, 128), tile8, payload],
        [swap_all(sent), s, many, coadd, cover, morph, mask_t],
        [tile3],
        "deblend_next",
    )
    (spectra,) = call(last_kernel, [(bands, owned, slots)], [swap_all(sent), s, many], (), "deblend_last")
    coadd = jnp.transpose(coadd.reshape(bands, owned, width), (1, 0, 2))
    return coadd, jnp.transpose(spectra, (1, 2, 0)), jnp.transpose(morph[:, :owned], (1, 0, 2))


def solution(mesh):
    in_specs = (
        P("epoch", None, None, "blend"),
        P("epoch", None, None, "blend"),
        P("epoch", None),
        P("blend", None, "epoch"),
        P("blend"),
        P("blend", None, None),
        P("blend", None, "epoch"),
    )
    out_specs = (P("blend", None, "epoch"), P("blend", None, None), P("blend", None, "epoch"))
    return jax.shard_map(
        on_device, mesh=mesh, in_specs=in_specs, out_specs=out_specs, check_vma=False
    )
```

```python
import jax
import jax.numpy as jnp
from jax import lax
from jax.experimental import pallas as pl
from jax.experimental.pallas import tpu as pltpu
from jax.sharding import PartitionSpec as P


VISIT_VMEM = 52 * 2**20
F32 = jnp.float32
VMEM = pl.BlockSpec(memory_space=pltpu.VMEM)
ANY = pl.BlockSpec(memory_space=pl.ANY)


def held_group(e, i):
    return 2 * ((e // 2 + 4 * (i % 2) - i // 2) % 8) + (e + i) % 2


def visit_kernel(first, flux_ref, prec_ref, live_ref, *rest):
    if first:
        outs, (live_out, flux_buf, prec_buf, live_buf, square, sems, live_sem) = rest[:8], rest[8:]
    else:
        outs, (flux_buf, prec_buf, sems) = rest[:8], rest[8:]
    e, i = lax.axis_index("epoch"), lax.axis_index("blend")
    odd = lax.rem(e + i, 2) == 1
    bands, visits, tiles = flux_buf.shape[:3]
    width = flux_buf.shape[4]
    base = 0 if first else bands
    copies = []
    if first:
        live_copy = pltpu.make_async_copy(live_ref, live_buf, live_sem)
        live_copy.start()
    for c in range(bands):
        row = []
        for v in range(visits):
            row.append(pltpu.make_async_copy(prec_ref.at[v, base + c], prec_buf.at[c, v], sems.at[0, c, v]))
            row.append(pltpu.make_async_copy(flux_ref.at[v, base + c], flux_buf.at[c, v], sems.at[1, c, v]))
        for copy in row:
            copy.start()
        copies.append(row)
    if first:
        live_copy.wait()
        square[...] = jnp.zeros(square.shape, F32)
        square[:visits, : 8 * tiles] = live_buf[...].astype(F32)
        turned = jnp.transpose(square[...])
        for v in range(visits):
            live_out[v] = jnp.broadcast_to(turned[: 8 * tiles, v : v + 1], (8 * tiles, 128)).reshape(tiles, 8, 128)
        live = live_out
    else:
        live = live_ref
    low_rows = lax.broadcasted_iota(jnp.int32, (8, 128), 0) < 4
    for c in range(bands):
        for copy in copies[c]:
            copy.wait()
        for j in range(tiles):
            pair = lax.rem(lax.bitwise_xor(lax.div(e, 2), j) + 4 * lax.rem(i, 2) + 8 - lax.div(i, 2), 8)
            lives = [live[v, pair] for v in range(visits)]
            x, y = 2 * (j % 2), j // 2
            (far0, far1), (at0, at1) = ((x, x + 1), (y, y)) if first else ((y, y), (x, x + 1))
            even, uneven = outs[2 * far0 + at0 // 2].at[at0 % 2], outs[2 * far1 + at1 // 2].at[at1 % 2]

            def lane_tile(l, _, c=c, pair=pair, lives=lives, even=even, uneven=uneven):
                lanes = pl.ds(pl.multiple_of(l * 128, 128), 128)
                num = wsum = None
                for v in range(visits):
                    w = prec_buf[c, v, pair, :, lanes].astype(F32) * lives[v]
                    n = w * flux_buf[c, v, pair, :, lanes].astype(F32)
                    num, wsum = (n, w) if v == 0 else (num + n, wsum + w)
                low = jnp.where(low_rows, num, pltpu.roll(wsum, 4, 0))
                high = jnp.where(low_rows, pltpu.roll(num, 4, 0), wsum)
                even[c, :, lanes] = jnp.where(odd, high, low)
                uneven[c, :, lanes] = jnp.where(odd, low, high)
                return 0

            lax.fori_loop(0, width // 128, lane_tile, 0, unroll=True)


def visit_sums(first, flux, prec, live):
    visits, bands, tiles, _, width = flux.shape
    half = bands // 2
    piece = jax.ShapeDtypeStruct((2, half, 8, width), F32)
    buf = pltpu.VMEM((half, visits, tiles, 8, width), flux.dtype)
    work = visits * half * tiles * 8 * width
    outs, scratch = [piece] * 8, [buf, buf, pltpu.SemaphoreType.DMA((2, half, visits))]
    if first:
        outs.append(jax.ShapeDtypeStruct((visits, tiles, 8, 128), F32))
        scratch[2:2] = [pltpu.VMEM(live.shape, live.dtype), pltpu.VMEM((128, 128), F32)]
        scratch.append(pltpu.SemaphoreType.DMA)
    return pl.pallas_call(
        lambda *refs: visit_kernel(first, *refs),
        out_shape=outs,
        in_specs=[ANY, ANY, ANY if first else VMEM],
        out_specs=[VMEM] * len(outs),
        scratch_shapes=scratch,
        compiler_params=pltpu.CompilerParams(vmem_limit_bytes=VISIT_VMEM),
        cost_estimate=pl.CostEstimate(flops=8 * work, bytes_accessed=4 * work, transcendentals=0),
        name="visit_first" if first else "visit_second",
    )(flux, prec, live)


def pass_kernel(a, b, c, d, low, high):
    low[...] = a[...] + b[...]
    high[...] = c[...] + d[...]


def pass_all_kernel(near0, mid0, far1, mid1, far0, near1, low, high):
    low[:2] = near0[...]
    low[2:] = mid0[...] + far1[...]
    high[:2] = mid1[...] + far0[...]
    high[2:] = near1[...]


def join_all_kernel(own0, own1, low, high, *outs):
    for n, out in enumerate(outs):
        out[...] = (own0, own1)[n // 2][n % 2] + low[n] + high[n]


def join_kernel(*refs):
    ins, outs = refs[:6], refs[6:]
    for n, out in enumerate(outs):
        a, b, c = ins[3 * (n // 2) : 3 * (n // 2) + 3]
        out[...] = a[n % 2] + b[n % 2] + c[n % 2]


def spread(tile, n):
    return jnp.broadcast_to(tile[:, n : n + 1], tile.shape)


def step_body(s, many, coadd_ref, cover_ref, morph, mask_ref, morph_out, resid_ref, payload_ref):
    halves, width = resid_ref.shape[0], resid_ref.shape[2]
    slots = mask_ref.shape[0]
    sb = [[spread(s, cc * slots + k) for cc in range(halves)] for k in range(slots)]
    steps = []
    for k in range(slots):
        sq = sb[k][0] * sb[k][0]
        for cc in range(1, halves):
            sq = sq + sb[k][cc] * sb[k][cc]
        sq = sq + pltpu.roll(sq, 4, 0)
        steps.append(1.0 / (1.0 + many * sq))

    def residual(ms, cc, lanes):
        model = sb[0][cc] * ms[0]
        for k in range(1, slots):
            model = model + sb[k][cc] * ms[k]
        return cover_ref[cc, :, lanes] * (coadd_ref[cc, :, lanes] - model)

    def lane_tile(l, _):
        lanes = pl.ds(pl.multiple_of(l * 128, 128), 128)
        ms = [morph[k, :, lanes] for k in range(slots)]
        rs = [residual(ms, cc, lanes) for cc in range(halves)]
        new = []
        for k in range(slots):
            grad = sb[k][0] * rs[0]
            for cc in range(1, halves):
                grad = grad + sb[k][cc] * rs[cc]
            grad = grad + pltpu.roll(grad, 4, 0)
            m = jnp.maximum(0.0, ms[k] + grad * steps[k]) * mask_ref[k, :, lanes]
            morph_out[k, :, lanes] = m
            new.append(m)
        for cc in range(halves):
            resid_ref[cc, :, lanes] = residual(new, cc, lanes)
        return 0

    lax.fori_loop(0, width // 128, lane_tile, 0, unroll=True)
    lane = lax.broadcasted_iota(jnp.int32, (8, 128), 1)
    total = jnp.zeros((8, 128), F32)
    rs = [resid_ref[cc] for cc in range(halves)]
    for k in range(slots):
        m = morph_out[k]
        for cc in range(halves):
            got = jnp.sum(m * rs[cc], axis=1, keepdims=True)
            total = jnp.where(lane == cc * slots + k, got, total)
        got = jnp.sum(m * m, axis=1, keepdims=True)
        total = jnp.where(lane == halves * slots + k, got, total)
    for n in range(payload_ref.shape[0]):
        payload_ref[n] = total


def spectra_step(s, many, arrived_ref, halves, slots):
    total = arrived_ref[0]
    for n in range(1, arrived_ref.shape[0]):
        total = total + arrived_ref[n]
    lane = lax.broadcasted_iota(jnp.int32, (8, 128), 1)
    norm = total
    for cc in range(halves):
        moved = pltpu.roll(total, 128 - (halves - cc) * slots, 1)
        norm = jnp.where((lane >= cc * slots) & (lane < (cc + 1) * slots), moved, norm)
    new = jnp.maximum(0.0, s + total / (1.0 + many * norm))
    return jnp.where(lane < halves * slots, new, 0.0)


def total_kernel(*refs):
    out = refs[8]
    half = out.shape[0] // 2
    for n in range(2):
        a, b, c, d = refs[4 * n : 4 * n + 4]
        out[n * half : (n + 1) * half] = (a[...] + b[...]) + (c[...] + d[...])


def first_kernel(
    sums_ref, mask_ref, morph_ref, s_ref, many_ref, coadd_ref, cover_ref, morph_out, payload_ref, resid_ref
):
    halves, width = coadd_ref.shape[0], coadd_ref.shape[2]
    low_rows = lax.broadcasted_iota(jnp.int32, (8, 128), 0) < 4

    def lane_tile(l, _):
        lanes = pl.ds(pl.multiple_of(l * 128, 128), 128)
        got = [sums_ref[n, :, lanes] for n in range(2 * halves)]
        for cc in range(halves):
            even, uneven = got[2 * cc], got[2 * cc + 1]
            num = jnp.where(low_rows, even, pltpu.roll(uneven, 4, 0))
            wsum = jnp.where(low_rows, pltpu.roll(even, 4, 0), uneven)
            below = 1.0 / (1.0 + wsum)
            coadd_ref[cc, :, lanes] = num * below
            cover_ref[cc, :, lanes] = wsum * below
        return 0

    lax.fori_loop(0, width // 128, lane_tile, 0, unroll=True)
    step_body(s_ref[...], many_ref[...], coadd_ref, cover_ref, morph_ref, mask_ref, morph_out, resid_ref, payload_ref)


def next_kernel(arrived_ref, s_ref, many_ref, coadd_ref, cover_ref, morph_ref, mask_ref, s_out, morph_out, payload_ref, resid_ref):
    halves, slots = coadd_ref.shape[0], mask_ref.shape[0]
    s = spectra_step(s_ref[...], many_ref[...], arrived_ref, halves, slots)
    s_out[...] = s
    step_body(s, many_ref[...], coadd_ref, cover_ref, morph_ref, mask_ref, morph_out, resid_ref, payload_ref)


def last_kernel(arrived_ref, s_ref, many_ref, out_ref):
    bands, owned, slots = out_ref.shape
    s = spectra_step(s_ref[...], many_ref[...], arrived_ref, bands // 2, slots)
    for c in range(bands):
        out_ref[c] = s[(c % 2) * owned : (c % 2 + 1) * owned, (c // 2) * slots : (c // 2 + 1) * slots]


def call(kernel, outs, args, scratch=()):
    return pl.pallas_call(
        kernel,
        out_shape=[jax.ShapeDtypeStruct(o, F32) for o in outs],
        in_specs=[VMEM] * len(args),
        out_specs=[VMEM] * len(outs),
        scratch_shapes=[pltpu.VMEM(s, F32) for s in scratch],
        compiler_params=pltpu.CompilerParams(vmem_limit_bytes=8 * 2**20),
        cost_estimate=pl.CostEstimate(flops=4_000_000, bytes_accessed=1_000_000, transcendentals=0),
    )(*args)


def on_device(visit_flux, visit_precision, visit_live, footprint, source_count, spectra_init, morphology_init):
    n_epoch, n_blend = lax.axis_size("epoch"), lax.axis_size("blend")
    owned, slots, width = footprint.shape
    bands = visit_flux.shape[2]
    halves = bands // 2

    def hop(a, m):
        return lax.ppermute(a, "epoch", [(e, e ^ m) for e in range(n_epoch)])


    tiled = lambda a: jnp.transpose(a, (0, 2, 1, 3)).reshape(a.shape[0], bands, a.shape[1] // 8, 8, a.shape[3])
    flux, prec = tiled(visit_flux), tiled(visit_precision)
    both_ways = lambda a, b, step: (hop(a, step), hop(b, 3 * step))
    *a, live = visit_sums(True, flux, prec, visit_live)
    b = visit_sums(False, flux, prec, live)
    a_far = both_ways(a[4], a[5], 1)
    b_far = both_ways(b[4], b[5], 4)
    b_near = both_ways(b[2], b[7], 4)
    two = (2, halves, 8, width)
    four = (4, halves, 8, width)
    a_last = both_ways(*call(pass_all_kernel, [four] * 2, [a[2], a[3], a_far[1], a[6], a_far[0], a[7]], ()), 1)
    b_last = both_ways(*call(pass_kernel, [two] * 2, [b[3], b_far[1], b[6], b_far[0]], ()), 4)

    piece = (halves, 8, width)
    home = [(e * n_blend + i, i * n_blend + held_group(e, i)) for e in range(n_epoch) for i in range(n_blend)]
    a = call(join_all_kernel, [piece] * 4, [a[0], a[1], *a_last], ())
    a = [a[0]] + [hop(a[m], 4 * m) for m in (2, 1, 3)]
    b = call(join_kernel, [piece] * 4, [b[0], b_near[0], b_last[1], b[1], b_near[1], b_last[0]], ())
    b = [b[0]] + [hop(b[m], m) for m in (2, 1, 3)]
    (total,) = call(total_kernel, [(bands, 8, width)], [*a, *b], ())
    sums = lax.ppermute(total, ("epoch", "blend"), home)

    source_live = (jnp.arange(slots, dtype=jnp.int32)[None, :] < source_count[:, None]).astype(F32)
    mask = footprint.astype(F32) * source_live[:, :, None]
    twice = lambda a: jnp.concatenate([a, a], axis=1)
    mask_t = twice(jnp.transpose(mask, (1, 0, 2)))
    morph_t = twice(jnp.transpose(morphology_init * mask, (1, 0, 2)))
    many = jnp.broadcast_to(jnp.tile(source_count.astype(F32), 2)[:, None], (8, 128))
    s = jnp.transpose(spectra_init.reshape(owned, slots, halves, 2), (3, 0, 2, 1)).reshape(2 * owned, halves * slots)
    s = jnp.pad(s, ((0, 0), (0, 128 - halves * slots)))

    tile3, tile8 = (halves, 8, width), (slots, 8, width)
    payload = (n_epoch, 8, 128)
    coadd, cover, morph, sent = call(
        first_kernel, [tile3, tile3, tile8, payload], [sums, mask_t, morph_t, s, many], [tile3]
    )
    swap_all = lambda a: lax.all_to_all(a, "epoch", split_axis=0, concat_axis=0, tiled=True)
    s, morph, sent = call(
        next_kernel, [(8, 128), tile8, payload], [swap_all(sent), s, many, coadd, cover, morph, mask_t], [tile3]
    )
    (spectra,) = call(last_kernel, [(bands, owned, slots)], [swap_all(sent), s, many], ())
    coadd = jnp.transpose(coadd.reshape(bands, owned, width), (1, 0, 2))
    return coadd, jnp.transpose(spectra, (1, 2, 0)), jnp.transpose(morph[:, :owned], (1, 0, 2))


def solution(mesh):
    in_specs = (
        P("epoch", None, None, "blend"),
        P("epoch", None, None, "blend"),
        P("epoch", None),
        P("blend", None, "epoch"),
        P("blend"),
        P("blend", None, None),
        P("blend", None, "epoch"),
    )
    out_specs = (P("blend", None, "epoch"), P("blend", None, None), P("blend", None, "epoch"))
    return jax.shard_map(on_device, mesh=mesh, in_specs=in_specs, out_specs=out_specs, check_vma=False)
```

```python
import jax
import jax.numpy as jnp
from jax import lax
from jax.experimental import pallas as pl
from jax.experimental.pallas import tpu as pltpu
from jax.sharding import PartitionSpec as P


VISIT_VMEM = 52 * 2**20
F32 = jnp.float32
VMEM = pl.BlockSpec(memory_space=pltpu.VMEM)
ANY = pl.BlockSpec(memory_space=pl.ANY)


PAIRS = (
    0x15742603,
    0x63521407,
    0x50123746,
    0x61274053,
    0x46231570,
    0x40375261,
    0x34261570,
    0x03624715,
    0x21654037,
    0x54306127,
    0x47120653,
    0x12705463,
    0x41567320,
    0x02763514,
    0x70154236,
    0x75340162,
)


def held_group(e, i):
    return 2 * (PAIRS[i] >> 4 * (e // 2) & 7) + (e + i) % 2


def visit_kernel(first, flux_ref, prec_ref, live_ref, *rest):
    if first:
        outs, (live_out, flux_buf, prec_buf, live_buf, square, sems, live_sem) = rest[:8], rest[8:]
    else:
        outs, (flux_buf, prec_buf, sems) = rest[:8], rest[8:]
    e, i = lax.axis_index("epoch"), lax.axis_index("blend")
    odd = lax.rem(e + i, 2) == 1
    held = jnp.int32(PAIRS[0])
    for n in range(1, len(PAIRS)):
        held = jnp.where(i == n, PAIRS[n], held)
    bands, visits, tiles = flux_buf.shape[:3]
    width = flux_buf.shape[4]
    base = 0 if first else bands
    copies = []
    if first:
        live_copy = pltpu.make_async_copy(live_ref, live_buf, live_sem)
        live_copy.start()
    for c in range(bands):
        row = []
        for v in range(visits):
            row.append(pltpu.make_async_copy(prec_ref.at[v, base + c], prec_buf.at[c, v], sems.at[0, c, v]))
            row.append(pltpu.make_async_copy(flux_ref.at[v, base + c], flux_buf.at[c, v], sems.at[1, c, v]))
        for copy in row:
            copy.start()
        copies.append(row)
    if first:
        live_copy.wait()
        square[...] = jnp.zeros(square.shape, F32)
        square[:visits, : 8 * tiles] = live_buf[...].astype(F32)
        turned = jnp.transpose(square[...])
        for v in range(visits):
            live_out[v] = jnp.broadcast_to(turned[: 8 * tiles, v : v + 1], (8 * tiles, 128)).reshape(tiles, 8, 128)
        live = live_out
    else:
        live = live_ref
    low_rows = lax.broadcasted_iota(jnp.int32, (8, 128), 0) < 4
    for c in range(bands):
        for copy in copies[c]:
            copy.wait()
        for j in range(tiles):
            pair = lax.bitwise_and(lax.shift_right_logical(held, 4 * lax.bitwise_xor(lax.div(e, 2), j)), 7)
            lives = [live[v, pair] for v in range(visits)]
            x, y = 2 * (j % 2), j // 2
            (far0, far1), (at0, at1) = ((x, x + 1), (y, y)) if first else ((y, y), (x, x + 1))
            even, uneven = outs[2 * far0 + at0 // 2].at[at0 % 2], outs[2 * far1 + at1 // 2].at[at1 % 2]

            def lane_tile(l, _, c=c, pair=pair, lives=lives, even=even, uneven=uneven):
                lanes = pl.ds(pl.multiple_of(l * 128, 128), 128)
                num = wsum = None
                for v in range(visits):
                    w = prec_buf[c, v, pair, :, lanes].astype(F32) * lives[v]
                    n = w * flux_buf[c, v, pair, :, lanes].astype(F32)
                    num, wsum = (n, w) if v == 0 else (num + n, wsum + w)
                low = jnp.where(low_rows, num, pltpu.roll(wsum, 4, 0))
                high = jnp.where(low_rows, pltpu.roll(num, 4, 0), wsum)
                even[c, :, lanes] = jnp.where(odd, high, low)
                uneven[c, :, lanes] = jnp.where(odd, low, high)
                return 0

            lax.fori_loop(0, width // 128, lane_tile, 0, unroll=True)


def visit_sums(first, flux, prec, live):
    visits, bands, tiles, _, width = flux.shape
    half = bands // 2
    piece = jax.ShapeDtypeStruct((2, half, 8, width), F32)
    buf = pltpu.VMEM((half, visits, tiles, 8, width), flux.dtype)
    work = visits * half * tiles * 8 * width
    outs, scratch = [piece] * 8, [buf, buf, pltpu.SemaphoreType.DMA((2, half, visits))]
    if first:
        outs.append(jax.ShapeDtypeStruct((visits, tiles, 8, 128), F32))
        scratch[2:2] = [pltpu.VMEM(live.shape, live.dtype), pltpu.VMEM((128, 128), F32)]
        scratch.append(pltpu.SemaphoreType.DMA)
    return pl.pallas_call(
        lambda *refs: visit_kernel(first, *refs),
        out_shape=outs,
        in_specs=[ANY, ANY, ANY if first else VMEM],
        out_specs=[VMEM] * len(outs),
        scratch_shapes=scratch,
        compiler_params=pltpu.CompilerParams(vmem_limit_bytes=VISIT_VMEM),
        cost_estimate=pl.CostEstimate(flops=8 * work, bytes_accessed=4 * work, transcendentals=0),
        name="visit_first" if first else "visit_second",
    )(flux, prec, live)


def pass_kernel(a, b, c, d, low, high):
    low[...] = a[...] + b[...]
    high[...] = c[...] + d[...]


def pass_all_kernel(near0, mid0, far1, mid1, far0, near1, low, high):
    low[:2] = near0[...]
    low[2:] = mid0[...] + far1[...]
    high[:2] = mid1[...] + far0[...]
    high[2:] = near1[...]


def join_all_kernel(own0, own1, low, high, *outs):
    for n, out in enumerate(outs):
        out[...] = (own0, own1)[n // 2][n % 2] + low[n] + high[n]


def join_kernel(*refs):
    ins, outs = refs[:6], refs[6:]
    for n, out in enumerate(outs):
        a, b, c = ins[3 * (n // 2) : 3 * (n // 2) + 3]
        out[...] = a[n % 2] + b[n % 2] + c[n % 2]


def spread(tile, n):
    return jnp.broadcast_to(tile[:, n : n + 1], tile.shape)


def step_body(s, many, coadd_ref, cover_ref, morph, mask_ref, morph_out, resid_ref, payload_ref):
    halves, width = resid_ref.shape[0], resid_ref.shape[2]
    slots = mask_ref.shape[0]
    sb = [[spread(s, cc * slots + k) for cc in range(halves)] for k in range(slots)]
    steps = []
    for k in range(slots):
        sq = sb[k][0] * sb[k][0]
        for cc in range(1, halves):
            sq = sq + sb[k][cc] * sb[k][cc]
        sq = sq + pltpu.roll(sq, 4, 0)
        steps.append(1.0 / (1.0 + many * sq))

    def residual(ms, cc, lanes):
        model = sb[0][cc] * ms[0]
        for k in range(1, slots):
            model = model + sb[k][cc] * ms[k]
        return cover_ref[cc, :, lanes] * (coadd_ref[cc, :, lanes] - model)

    def lane_tile(l, _):
        lanes = pl.ds(pl.multiple_of(l * 128, 128), 128)
        ms = [morph[k, :, lanes] for k in range(slots)]
        rs = [residual(ms, cc, lanes) for cc in range(halves)]
        new = []
        for k in range(slots):
            grad = sb[k][0] * rs[0]
            for cc in range(1, halves):
                grad = grad + sb[k][cc] * rs[cc]
            grad = grad + pltpu.roll(grad, 4, 0)
            m = jnp.maximum(0.0, ms[k] + grad * steps[k]) * mask_ref[k, :, lanes]
            morph_out[k, :, lanes] = m
            new.append(m)
        for cc in range(halves):
            resid_ref[cc, :, lanes] = residual(new, cc, lanes)
        return 0

    lax.fori_loop(0, width // 128, lane_tile, 0, unroll=True)
    lane = lax.broadcasted_iota(jnp.int32, (8, 128), 1)
    total = jnp.zeros((8, 128), F32)
    rs = [resid_ref[cc] for cc in range(halves)]
    for k in range(slots):
        m = morph_out[k]
        for cc in range(halves):
            got = jnp.sum(m * rs[cc], axis=1, keepdims=True)
            total = jnp.where(lane == cc * slots + k, got, total)
        got = jnp.sum(m * m, axis=1, keepdims=True)
        total = jnp.where(lane == halves * slots + k, got, total)
    for n in range(payload_ref.shape[0]):
        payload_ref[n] = total


def spectra_step(s, many, arrived_ref, halves, slots):
    total = arrived_ref[0]
    for n in range(1, arrived_ref.shape[0]):
        total = total + arrived_ref[n]
    lane = lax.broadcasted_iota(jnp.int32, (8, 128), 1)
    norm = total
    for cc in range(halves):
        moved = pltpu.roll(total, 128 - (halves - cc) * slots, 1)
        norm = jnp.where((lane >= cc * slots) & (lane < (cc + 1) * slots), moved, norm)
    new = jnp.maximum(0.0, s + total / (1.0 + many * norm))
    return jnp.where(lane < halves * slots, new, 0.0)


def total_kernel(*refs):
    out = refs[8]
    half = out.shape[0] // 2
    for n in range(2):
        a, b, c, d = refs[4 * n : 4 * n + 4]
        out[n * half : (n + 1) * half] = (a[...] + b[...]) + (c[...] + d[...])


def first_kernel(
    sums_ref, mask_ref, morph_ref, s_ref, many_ref, coadd_ref, cover_ref, morph_out, payload_ref, resid_ref
):
    halves, width = coadd_ref.shape[0], coadd_ref.shape[2]
    low_rows = lax.broadcasted_iota(jnp.int32, (8, 128), 0) < 4

    def lane_tile(l, _):
        lanes = pl.ds(pl.multiple_of(l * 128, 128), 128)
        got = [sums_ref[n, :, lanes] for n in range(2 * halves)]
        for cc in range(halves):
            even, uneven = got[2 * cc], got[2 * cc + 1]
            num = jnp.where(low_rows, even, pltpu.roll(uneven, 4, 0))
            wsum = jnp.where(low_rows, pltpu.roll(even, 4, 0), uneven)
            below = 1.0 / (1.0 + wsum)
            coadd_ref[cc, :, lanes] = num * below
            cover_ref[cc, :, lanes] = wsum * below
        return 0

    lax.fori_loop(0, width // 128, lane_tile, 0, unroll=True)
    step_body(s_ref[...], many_ref[...], coadd_ref, cover_ref, morph_ref, mask_ref, morph_out, resid_ref, payload_ref)


def next_kernel(arrived_ref, s_ref, many_ref, coadd_ref, cover_ref, morph_ref, mask_ref, s_out, morph_out, payload_ref, resid_ref):
    halves, slots = coadd_ref.shape[0], mask_ref.shape[0]
    s = spectra_step(s_ref[...], many_ref[...], arrived_ref, halves, slots)
    s_out[...] = s
    step_body(s, many_ref[...], coadd_ref, cover_ref, morph_ref, mask_ref, morph_out, resid_ref, payload_ref)


def last_kernel(arrived_ref, s_ref, many_ref, out_ref):
    bands, owned, slots = out_ref.shape
    s = spectra_step(s_ref[...], many_ref[...], arrived_ref, bands // 2, slots)
    for c in range(bands):
        out_ref[c] = s[(c % 2) * owned : (c % 2 + 1) * owned, (c // 2) * slots : (c // 2 + 1) * slots]


def call(kernel, outs, args, scratch=()):
    return pl.pallas_call(
        kernel,
        out_shape=[jax.ShapeDtypeStruct(o, F32) for o in outs],
        in_specs=[VMEM] * len(args),
        out_specs=[VMEM] * len(outs),
        scratch_shapes=[pltpu.VMEM(s, F32) for s in scratch],
        compiler_params=pltpu.CompilerParams(vmem_limit_bytes=8 * 2**20),
        cost_estimate=pl.CostEstimate(flops=4_000_000, bytes_accessed=1_000_000, transcendentals=0),
    )(*args)


def on_device(visit_flux, visit_precision, visit_live, footprint, source_count, spectra_init, morphology_init):
    n_epoch, n_blend = lax.axis_size("epoch"), lax.axis_size("blend")
    owned, slots, width = footprint.shape
    bands = visit_flux.shape[2]
    halves = bands // 2

    def hop(a, m):
        return lax.ppermute(a, "epoch", [(e, e ^ m) for e in range(n_epoch)])


    tiled = lambda a: jnp.transpose(a, (0, 2, 1, 3)).reshape(a.shape[0], bands, a.shape[1] // 8, 8, a.shape[3])
    flux, prec = tiled(visit_flux), tiled(visit_precision)
    both_ways = lambda a, b, step: (hop(a, step), hop(b, 3 * step))
    *a, live = visit_sums(True, flux, prec, visit_live)
    b = visit_sums(False, flux, prec, live)
    a_far = both_ways(a[4], a[5], 1)
    b_far = both_ways(b[4], b[5], 4)
    b_near = both_ways(b[2], b[7], 4)
    two = (2, halves, 8, width)
    four = (4, halves, 8, width)
    a_last = both_ways(*call(pass_all_kernel, [four] * 2, [a[2], a[3], a_far[1], a[6], a_far[0], a[7]], ()), 1)
    b_last = both_ways(*call(pass_kernel, [two] * 2, [b[3], b_far[1], b[6], b_far[0]], ()), 4)

    piece = (halves, 8, width)
    home = [(e * n_blend + i, i * n_blend + held_group(e, i)) for e in range(n_epoch) for i in range(n_blend)]
    a = call(join_all_kernel, [piece] * 4, [a[0], a[1], *a_last], ())
    a = [a[0]] + [hop(a[m], 4 * m) for m in (2, 1, 3)]
    b = call(join_kernel, [piece] * 4, [b[0], b_near[0], b_last[1], b[1], b_near[1], b_last[0]], ())
    b = [b[0]] + [hop(b[m], m) for m in (1, 3, 2)]
    (total,) = call(total_kernel, [(bands, 8, width)], [*a, *b], ())
    sums = lax.ppermute(total, ("epoch", "blend"), home)

    source_live = (jnp.arange(slots, dtype=jnp.int32)[None, :] < source_count[:, None]).astype(F32)
    mask = footprint.astype(F32) * source_live[:, :, None]
    twice = lambda a: jnp.concatenate([a, a], axis=1)
    mask_t = twice(jnp.transpose(mask, (1, 0, 2)))
    morph_t = twice(jnp.transpose(morphology_init * mask, (1, 0, 2)))
    many = jnp.broadcast_to(jnp.tile(source_count.astype(F32), 2)[:, None], (8, 128))
    s = jnp.transpose(spectra_init.reshape(owned, slots, halves, 2), (3, 0, 2, 1)).reshape(2 * owned, halves * slots)
    s = jnp.pad(s, ((0, 0), (0, 128 - halves * slots)))

    tile3, tile8 = (halves, 8, width), (slots, 8, width)
    payload = (n_epoch, 8, 128)
    coadd, cover, morph, sent = call(
        first_kernel, [tile3, tile3, tile8, payload], [sums, mask_t, morph_t, s, many], [tile3]
    )
    swap_all = lambda a: lax.all_to_all(a, "epoch", split_axis=0, concat_axis=0, tiled=True)
    s, morph, sent = call(
        next_kernel, [(8, 128), tile8, payload], [swap_all(sent), s, many, coadd, cover, morph, mask_t], [tile3]
    )
    (spectra,) = call(last_kernel, [(bands, owned, slots)], [swap_all(sent), s, many], ())
    coadd = jnp.transpose(coadd.reshape(bands, owned, width), (1, 0, 2))
    return coadd, jnp.transpose(spectra, (1, 2, 0)), jnp.transpose(morph[:, :owned], (1, 0, 2))


def solution(mesh):
    in_specs = (
        P("epoch", None, None, "blend"),
        P("epoch", None, None, "blend"),
        P("epoch", None),
        P("blend", None, "epoch"),
        P("blend"),
        P("blend", None, None),
        P("blend", None, "epoch"),
    )
    out_specs = (P("blend", None, "epoch"), P("blend", None, None), P("blend", None, "epoch"))
    return jax.shard_map(on_device, mesh=mesh, in_specs=in_specs, out_specs=out_specs, check_vma=False)
```
